512 devices in a mesh: groups: 2 (over y), rows: 16 (over z), cols: 8 (over x), sub: 2 (over core).
Axes of the slice: x: 8, y: 2, z: 16, core: 2. Of those that a mesh axis runs over, the one named last changes fastest.
The devices are a block of a 8x8x16 slice.
Arguments:
- stored_vectors: bfloat16 [3072, 131072], P(('cols', 'sub'), ('groups', 'rows')), parts along dimension 1, may hold values from -0.59765625 to 0.59765625
- previous_columns: bfloat16 [131072, 256], P(('groups', 'rows', 'cols', 'sub')), parts along dimension 0, may hold values from -3 to 3
- pivots: int32 [512], P('groups'), parts along dimension 0, may hold values from 0 to 65535, as said below
- diagonal: float32 [131072], P(('groups', 'rows', 'cols', 'sub')), parts along dimension 0, may hold values from 2 to 32
- ket_blocks: bfloat16 [2048, 128, 256], P(('groups', 'rows', 'cols', 'sub')), parts along dimension 0, may hold values from -6 to 6
- shell_tags: int32 [2048, 128], P(('groups', 'rows', 'cols', 'sub')), parts along dimension 0, may hold values from 0 to 3
- target_blocks: int32 [512, 4], P('groups'), parts along dimension 0, may hold values from 0 to 511, as said below
- block_counts: int32 [512], P('groups'), parts along dimension 0, may hold values from 0 to 4, as said below
- shell_norms: float32 [4], replicated, may hold values from 0.5 to 2
Outputs:
- new_vectors: bfloat16 [131072, 256], P(('groups', 'rows', 'cols', 'sub')), parts along dimension 0
- diag_out: float32 [131072], P(('groups', 'rows', 'cols', 'sub')), parts along dimension 0
- next_columns: bfloat16 [131072, 256], P(('groups', 'rows', 'cols', 'sub')), parts along dimension 0
The draws below stay inside these ranges and needn't reach their ends.
There are 2 independent parts, one for each index of `groups`. The reference program is written for one: setup_inputs(seed, part) draws one part's arguments, and reference() takes and returns one part's arrays. A program takes and returns all parts, laid end to end along the dimension named above; an argument that names none is the same for every part. Nothing has to cross between parts.
Inputs may be any that keep to these rules, and one draw needn't show every extreme that they name: `pivots`: 256 distinct AO pairs. `target_blocks`: the used slots of all owners name every block of the 512 blocks exactly once; a used slot's block lies on a device with the owner's cols and sub indices (blocks g * 2 to g * 2 + 1 lie on the device of linear index g, rows slowest; owner o is the device of linear index o). At most 1 of one owner's used slots go to one device, and some owner reaches that in every draw. Entries of unused slots are arbitrary blocks. `block_counts`: some owner uses all 4 slots in every draw.
All inputs are finite; a program needn't handle non-finite values.
Results may differ from the reference program's by a relative error of at most 0.0004.
Values may be sent and summed in bfloat16 or wider, within the bound.
A program may use at most 64 MiB of HBM per device.

```python
import math
import jax
import jax.numpy as jnp
from jax import lax

K = 3072
B = 256
BLK = 128
BLOCKS_DEV = 2
SHELL_TYPES = 4
CAP = 4
OWNERS = 256
PAIRS = 65536
N_ROWS = 16
N_COLS = 8
N_SUB = 2


def layout_draw(key):
    band_count = N_ROWS
    column = N_COLS * N_SUB
    per_device = BLOCKS_DEV
    slot_count = 2 * BLOCKS_DEV
    base = jax.random.fold_in(key, 11)
    keys = jax.random.split(base, 4)
    ranks = jnp.arange(band_count, dtype=jnp.int32)
    rank_counts = jnp.where(ranks == 0, slot_count, jnp.where(ranks == 1, 0, per_device)).astype(jnp.int32)
    rank_starts = (jnp.cumsum(rank_counts) - rank_counts).astype(jnp.int32)
    order = jax.vmap(lambda sub_key: jax.random.permutation(sub_key, band_count))(jax.random.split(keys[0], column)).astype(jnp.int32)
    lines = jnp.arange(column, dtype=jnp.int32)[:, None]
    counts = jnp.zeros((column, band_count), jnp.int32).at[lines, order].set(jnp.broadcast_to(rank_counts, (column, band_count)))
    starts = jnp.zeros((column, band_count), jnp.int32).at[lines, order].set(jnp.broadcast_to(rank_starts, (column, band_count)))
    total = band_count * per_device
    receiver_order = jax.vmap(lambda sub_key: jax.random.permutation(sub_key, band_count))(jax.random.split(keys[1], column)).astype(jnp.int32)
    within_order = jax.vmap(lambda sub_key: jax.random.permutation(sub_key, per_device))(jax.random.split(keys[2], column)).astype(jnp.int32)
    slots = jnp.arange(slot_count, dtype=jnp.int32)
    position = jnp.minimum(starts[:, :, None] + slots[None, None, :], total - 1)
    receiver_spread = jnp.broadcast_to(receiver_order[:, None, :], (column, band_count, band_count))
    receiver = jnp.take_along_axis(receiver_spread, position % band_count, axis=2)
    within_spread = jnp.broadcast_to(within_order[:, None, :], (column, band_count, per_device))
    within = jnp.take_along_axis(within_spread, position // band_count, axis=2)
    target = (receiver * column + jnp.arange(column, dtype=jnp.int32)[:, None, None]) * per_device + within
    filler = jax.random.randint(keys[3], (column, band_count, slot_count), 0, band_count * column * per_device).astype(jnp.int32)
    valid = slots[None, None, :] < counts[:, :, None]
    target = jnp.where(valid, target, filler)
    target = jnp.transpose(target, (1, 0, 2)).reshape(band_count * column, slot_count)
    owner_counts = jnp.transpose(counts, (1, 0)).reshape(band_count * column)
    return (target.astype(jnp.int32), owner_counts.astype(jnp.int32))


def draw_target_blocks(key, part):
    return layout_draw(key)[0]


def draw_block_counts(key, part):
    return layout_draw(key)[1]


def draw_pivots(key, part):
    chosen = jax.random.permutation(jax.random.fold_in(key, 5), PAIRS)
    return chosen[:B].astype(jnp.int32)


def place_ends(entries, key, smallest, largest):
    longest = entries.shape.index(max(entries.shape))
    spots = []
    for shift in (0, 1):
        where = [jax.random.randint(jax.random.fold_in(key, axis), (), 0, length) for axis, length in enumerate(entries.shape)]
        where[longest] = (where[longest] + shift) % entries.shape[longest]
        spots.append(tuple(where))
    return entries.at[spots[0]].set(smallest).at[spots[1]].set(largest)


def block_levels(rng, extent, cuts, low, high):
    gain = 1.0
    for dim, shards_of in cuts:
        draws = jax.random.uniform(jax.random.fold_in(jax.random.fold_in(rng, 6), dim), (shards_of,), jnp.float32, low / len(cuts), high / len(cuts))
        gain = gain * jnp.repeat(jnp.exp(draws), extent[dim] // shards_of).reshape((-1,) + (1,) * (len(extent) - 1 - dim))
    return gain


def centred(own_key, extent, scale, most, pieces=(), kind=jnp.bfloat16):
    entries = scale * jax.random.normal(own_key, extent, jnp.float32)
    if pieces:
        entries = entries * block_levels(own_key, extent, pieces, -0.22, 0.18)
    return jnp.clip(entries, -most, most).astype(kind)


def setup_inputs(seed: int = 0, part: int = 0) -> dict:
    seeds = jax.random.split(jax.random.key(seed), 10)
    part_keys = jax.random.split(jax.random.fold_in(seeds[9], part), 10)
    return {
        "stored_vectors": centred(part_keys[0], (K, PAIRS), 0.1, 0.59765625, ((0, 16), (1, 16))),
        "previous_columns": centred(part_keys[1], (PAIRS, B), 0.5, 3.0, ((0, 256),)),
        "pivots": draw_pivots(jax.random.fold_in(jax.random.fold_in(seeds[9], part), 71), part),
        "diagonal": jnp.clip(jnp.exp(math.log(32.0) - 2.7725887 * jax.random.uniform(part_keys[3], (PAIRS,), jnp.float32) ** block_levels(part_keys[3], (PAIRS,), ((0, 256),), -0.2, 0.2)), 2.0, 32.0),
        "ket_blocks": centred(part_keys[4], (OWNERS * CAP, BLK, B), 1.0, 6.0, ((0, 256),)),
        "shell_tags": place_ends(jax.random.randint(part_keys[5], (OWNERS * CAP, BLK), 0, SHELL_TYPES), jax.random.fold_in(part_keys[5], 1), 0, SHELL_TYPES - 1).astype(jnp.int32),
        "target_blocks": draw_target_blocks(jax.random.fold_in(jax.random.fold_in(seeds[9], part), 71), part),
        "block_counts": draw_block_counts(jax.random.fold_in(jax.random.fold_in(seeds[9], part), 71), part),
        "shell_norms": jnp.clip(jnp.exp(jax.random.uniform(seeds[8], (SHELL_TYPES,), jnp.float32, math.log(0.5), math.log(2.0))), 0.5, 2.0),
    }


def reference(stored_vectors, previous_columns, pivots, diagonal, ket_blocks, shell_tags, target_blocks, block_counts, shell_norms):
    kinds = jnp.arange(shell_norms.shape[0], dtype=jnp.int32)
    factor = lax.optimization_barrier(jnp.sum(jnp.where(shell_tags[..., None] == kinds, shell_norms, jnp.float32(0.0)), axis=-1))
    fresh = (ket_blocks.astype(jnp.float32) * factor[..., None]).astype(jnp.bfloat16)
    slots = jnp.arange(CAP, dtype=jnp.int32)
    valid = slots[None, :] < block_counts[:, None]
    blocks_total = PAIRS // BLK
    placing = jnp.where(valid, target_blocks, blocks_total).reshape(-1).astype(jnp.int32)
    placed = jnp.zeros((blocks_total, BLK, B), jnp.bfloat16).at[placing].set(fresh, mode='drop')
    next_columns = placed.reshape(PAIRS, B)
    pivot_rows = stored_vectors[:, pivots]
    groups_count = N_COLS * N_SUB
    width = K // groups_count
    product = jnp.zeros((PAIRS, B), jnp.float32)
    for group in range(groups_count):
        block_vectors = stored_vectors[group * width:(group + 1) * width]
        block_pivots = pivot_rows[group * width:(group + 1) * width]
        partial_sum = jnp.dot(block_vectors.T, block_pivots, preferred_element_type=jnp.float32)
        product = product + partial_sum
    residual_cols = previous_columns.astype(jnp.float32) - product
    pivot_diag = diagonal[pivots]
    scaled = residual_cols / jnp.sqrt(pivot_diag)[None, :]
    new_vectors = scaled.astype(jnp.bfloat16)
    diag_out = diagonal - lax.optimization_barrier(jnp.sum(scaled * scaled, axis=1))
    return (new_vectors, diag_out, next_columns)
```

```python
import functools

import jax
import jax.numpy as jnp
from jax import lax
from jax.experimental import pallas as pl
from jax.experimental.pallas import tpu as pltpu
from jax.sharding import PartitionSpec as P

MESH = pl.DeviceIdType.MESH
LANES = 128
PIVOT_GROUPS = 4
DIAG_PARTS = 3
BEFORE = 2


def kernel(
    nz,
    nx,
    v_hbm,
    prev_hbm,
    piv_ref,
    diag_ref,
    ket_hbm,
    tags_ref,
    tgt_ref,
    cnt_ref,
    norms_ref,
    new_ref,
    dout_ref,
    next_ref,
    v_ref,
    prev_ref,
    ket_ref,
    fresh_ref,
    hot_ref,
    pick_ref,
    rx1_ref,
    pful_ref,
    snd_ref,
    loc_ref,
    rsib_ref,
    rxr_ref,
    rxl_ref,
    k0_ref,
    krr_ref,
    krl_ref,
    dsnd_ref,
    dsib_ref,
    dsum_ref,
    drx_ref,
    prevt_ref,
    rs_ref,
    outt_ref,
    vsem,
    lsem,
    p1s,
    p1r,
    p2s,
    p2r,
    d2s,
    d2r,
    xrs,
    xrr,
    xls,
    xlr,
    krs,
    krq,
    kls,
    klq,
    dss,
    dsr,
    dxs,
    dxr,
):
    f32, bf16 = jnp.float32, jnp.bfloat16
    depth, band = v_ref.shape
    rows_here, batch = prev_ref.shape
    slots, block_rows = ket_ref.shape[0], ket_ref.shape[1]
    blocks = rows_here // block_rows
    chunk = batch // nz
    per = nz // PIVOT_GROUPS
    grows = per * chunk
    half = nx // 2
    r, c, s = lax.axis_index("rows"), lax.axis_index("cols"), lax.axis_index("sub")
    other = 1 - s
    device = (r * nx + c) * 2 + s
    right, left = lax.rem(c + 1, nx), lax.rem(c + nx - 1, nx)
    up, down = lax.rem(r + 1, nz), lax.rem(r + nz - 1, nz)

    def zpeer(k):
        return lax.rem(r + k, nz)

    def xpeer(k):
        return lax.rem(c + k, nx)

    barrier = pltpu.get_barrier_semaphore()
    by_reach = sorted(range(1, nz), key=lambda k: -min(k, nz - k))
    for k in by_reach:
        pl.semaphore_signal(barrier, inc=1, device_id={"rows": zpeer(k)}, device_id_type=MESH)
    for k in range(1, nx):
        pl.semaphore_signal(barrier, inc=1, device_id={"cols": xpeer(k)}, device_id_type=MESH)
    pl.semaphore_signal(barrier, inc=1, device_id={"sub": other}, device_id_type=MESH)

    pieces = 4
    width = band // pieces
    vload = [
        pltpu.make_async_copy(
            v_hbm.at[:, pl.ds(i * width, width)], v_ref.at[:, pl.ds(i * width, width)], vsem.at[i]
        )
        for i in range(pieces)
    ]
    for copy in vload:
        copy.start()
    ketload = pltpu.make_async_copy(ket_hbm, ket_ref, lsem.at[0])
    ketload.start()
    prevload = pltpu.make_async_copy(prev_hbm, prev_ref, lsem.at[1])
    prevload.start()

    pivot_cols = jnp.transpose(jnp.broadcast_to(piv_ref[...], (LANES, batch)))
    lane = lax.broadcasted_iota(jnp.int32, (batch, LANES), 1)
    in_band = pivot_cols - r * band - lane
    for t in range(band // LANES):
        hot = jnp.where(in_band == t * LANES, f32(1.0), f32(0.0)).astype(bf16)
        hot_ref[:, t * LANES : (t + 1) * LANES] = hot
    in_device = pivot_cols - device * rows_here - lane
    found = jnp.zeros((batch, LANES), f32)
    for t in range(rows_here // LANES):
        row = diag_ref[:, t * LANES : (t + 1) * LANES]
        found = found + jnp.where(in_device == t * LANES, row, f32(0.0))
    own_diag = jnp.sum(found, axis=1, keepdims=True)
    part_hi = own_diag.astype(bf16).astype(f32)
    part_mid = (own_diag - part_hi).astype(bf16).astype(f32)
    part_lo = own_diag - part_hi - part_mid
    spare = pick_ref.shape[1] - depth
    place = lax.broadcasted_iota(jnp.int32, (batch, spare), 1)
    extra = jnp.where(place == 0, part_hi, f32(0.0))
    extra = jnp.where(place == 1, part_mid, extra)
    extra = jnp.where(place == 2, part_lo, extra)
    pick_ref[:, depth:] = extra.astype(bf16)
    picked = jnp.zeros((batch, depth), f32)
    for i in range(pieces):
        vload[i].wait()
        span = slice(i * width, (i + 1) * width)
        picked = picked + lax.dot_general(
            hot_ref[:, span], v_ref[:, span], (((1,), (1,)), ((), ())), preferred_element_type=f32
        )
    pick_ref[:, :depth] = picked.astype(bf16)

    pl.semaphore_wait(barrier, nz - 1 + nx - 1 + 1)

    sends = []

    def push(src, dst, send_sem, recv_sem, to):
        copy = pltpu.make_async_remote_copy(
            src_ref=src,
            dst_ref=dst,
            send_sem=send_sem,
            recv_sem=recv_sem,
            device_id=to,
            device_id_type=MESH,
        )
        copy.start()
        sends.append(copy)

    def arrive(dst, send_sem, recv_sem, to):
        pltpu.make_async_remote_copy(
            src_ref=dst,
            dst_ref=dst,
            send_sem=send_sem,
            recv_sem=recv_sem,
            device_id=to,
            device_id_type=MESH,
        ).wait_recv()

    for k in by_reach:
        to = zpeer(k)
        start = pl.multiple_of(to * chunk, chunk)
        push(
            pick_ref.at[pl.ds(start, chunk), :], rx1_ref.at[k], p1s.at[k], p1r.at[k], {"rows": to}
        )

    ketload.wait()
    tags = tags_ref[...]
    factor = jnp.zeros(tags.shape, f32)
    for kind in range(norms_ref.shape[0]):
        factor = jnp.where(tags == kind, norms_ref[kind], factor)
    for t in range(slots):
        column = jnp.transpose(jnp.broadcast_to(factor[t : t + 1, :], (LANES, block_rows)))
        for h in range(batch // LANES):
            span = slice(h * LANES, (h + 1) * LANES)
            fresh_ref[t, :, span] = (ket_ref[t, :, span].astype(f32) * column).astype(bf16)
    prevload.wait()
    prevt_ref[...] = jnp.transpose(prev_ref[...].astype(f32))

    targets = [jnp.where(t < cnt_ref[device], tgt_ref[t, device], -1) for t in range(slots)]

    def with_own(value, reach, w):
        block = ((lax.rem(r + reach + nz, nz) * nx + c) * 2 + s) * blocks + w
        for t in range(slots):
            value = jnp.where(targets[t] == block, fresh_ref[t], value)
        return value

    zr, zl = nz // 2, nz - 1 - nz // 2

    def ket_right(i):
        if i >= zr:
            return
        for w in range(blocks):
            if i == 0:
                src = k0_ref.at[0, w]
                src[...] = with_own(jnp.zeros(fresh_ref.shape[1:], bf16), zr, w)
            else:
                src = krr_ref.at[i - 1, w]
                arrive(src, krs.at[i - 1, w], krq.at[i - 1, w], {"rows": up})
                src[...] = with_own(src[...], zr - i, w)
            push(src, krr_ref.at[i, w], krs.at[i, w], krq.at[i, w], {"rows": up})

    def ket_left(i):
        if i >= zl:
            return
        for w in range(blocks):
            if i == 0:
                src = k0_ref.at[1, w]
                src[...] = with_own(jnp.zeros(fresh_ref.shape[1:], bf16), -zl, w)
            else:
                src = krl_ref.at[i - 1, w]
                arrive(src, kls.at[i - 1, w], klq.at[i - 1, w], {"rows": down})
                src[...] = with_own(src[...], i - zl, w)
            push(src, krl_ref.at[i, w], kls.at[i, w], klq.at[i, w], {"rows": down})

    def ket(i):
        ket_right(i)
        ket_left(i)

    def ket_last():
        for w in range(blocks):
            arrive(krr_ref.at[zr - 1, w], krs.at[zr - 1, w], krq.at[zr - 1, w], {"rows": up})
            arrive(krl_ref.at[zl - 1, w], kls.at[zl - 1, w], klq.at[zl - 1, w], {"rows": down})
            both = krr_ref[zr - 1, w].astype(f32) + krl_ref[zl - 1, w].astype(f32)
            next_ref[w * block_rows : (w + 1) * block_rows, :] = with_own(both.astype(bf16), 0, w)

    own = pl.multiple_of(r * chunk, chunk)
    total = pick_ref[pl.ds(own, chunk), :].astype(f32)
    for k in range(1, nz):
        arrive(rx1_ref.at[k], p1s.at[k], p1r.at[k], {"rows": zpeer(k)})
        total = total + rx1_ref[k].astype(f32)
    mine = slice(BEFORE * chunk, (BEFORE + 1) * chunk)
    pful_ref[mine, :] = total.astype(bf16)
    for k in reversed(by_reach):
        at = ((BEFORE - k) % nz) * chunk
        push(
            pful_ref.at[mine, :],
            pful_ref.at[pl.ds(at, chunk), :],
            p2s.at[k],
            p2r.at[k],
            {"rows": zpeer(k)},
        )

    order = [(half - p // 2) if p % 2 == 0 else (half + (p + 1) // 2) % nx for p in range(nx)]
    where_is = {rel: p for p, rel in enumerate(order)}
    members = [0, 1, PIVOT_GROUPS - 1] + list(range(2, PIVOT_GROUPS - 1))
    pairs = nx // 2

    def columns_of(p, core):
        rel = order[p]
        return pl.multiple_of((xpeer(rel) * 2 + core) * rows_here, rows_here)

    def multiply(g):
        first = members[g] * per
        for p in range(first, first + per):
            if p != BEFORE:
                k = (BEFORE - p) % nz
                at = pful_ref.at[pl.ds(p * chunk, chunk), :]
                arrive(at, p2s.at[k], p2r.at[k], {"rows": zpeer(k)})
        lhs = pful_ref[first * chunk : first * chunk + grows, :depth]
        for m in range(pairs):
            for p in (2 * m, 2 * m + 1):
                snd_ref[g, p] = jnp.dot(
                    lhs, v_ref[:, pl.ds(columns_of(p, other), rows_here)], preferred_element_type=f32
                )
            span = pl.ds(2 * m, 2)
            push(
                snd_ref.at[g, span], rsib_ref.at[g, span], d2s.at[g, m], d2r.at[g, m], {"sub": other}
            )
        for p in range(nx):
            loc_ref[g, p] = jnp.dot(
                lhs, v_ref[:, pl.ds(columns_of(p, s), rows_here)], preferred_element_type=f32
            )

    met = set()

    def chip_part(g, p):
        m = p // 2
        if (g, m) not in met:
            met.add((g, m))
            arrive(rsib_ref.at[g, pl.ds(2 * m, 2)], d2s.at[g, m], d2r.at[g, m], {"sub": other})
        return loc_ref[g, p] + rsib_ref[g, p]

    def hops(g):
        longer = list(range(half, 0, -1)), list(range(nx - half + 1, nx))
        shorter = list(range(half - 1, 0, -1)), list(range(nx - half, nx))
        return longer if g % 2 == 0 else shorter

    def x_step(g, i):
        for way, (buf, ss, rs, to) in enumerate(
            ((rxr_ref, xrs, xrr, right), (rxl_ref, xls, xlr, left))
        ):
            path = hops(g)[way]
            if i >= len(path):
                continue
            p = where_is[path[i]]
            value = chip_part(g, p)
            if i > 0:
                arrive(buf.at[g, i - 1], ss.at[g, i - 1], rs.at[g, i - 1], {"cols": to})
                value = value + buf[g, i - 1]
            loc_ref[g, p] = value
            push(loc_ref.at[g, p], buf.at[g, i], ss.at[g, i], rs.at[g, i], {"cols": to})

    squares = [jnp.zeros((chunk, rows_here), f32)]

    def finish(g):
        value = chip_part(g, where_is[0])
        for way, (buf, ss, rs, to) in enumerate(
            ((rxr_ref, xrs, xrr, right), (rxl_ref, xls, xlr, left))
        ):
            last = len(hops(g)[way]) - 1
            arrive(buf.at[g, last], ss.at[g, last], rs.at[g, last], {"cols": to})
            value = value + buf[g, last]
        for q in range(per):
            p = members[g] * per + q
            at = pl.multiple_of(lax.rem(p + r + nz - BEFORE, nz) * chunk, chunk)
            scale = rs_ref[p * chunk : (p + 1) * chunk, :]
            scale = jnp.concatenate([scale] * (rows_here // LANES), axis=1)
            scaled = (prevt_ref[pl.ds(at, chunk), :] - value[q * chunk : (q + 1) * chunk]) * scale
            squares[0] = squares[0] + scaled * scaled
            outt_ref[pl.ds(at, chunk), :] = scaled

    def diag_to_sibling():
        tile = depth // LANES
        at = depth - tile * LANES
        turned = jnp.transpose(pful_ref[:, tile * LANES : (tile + 1) * LANES].astype(f32))
        dsnd_ref[...] = (
            turned[at : at + 1, :] + turned[at + 1 : at + 2, :] + turned[at + 2 : at + 3, :]
        )
        push(dsnd_ref, dsib_ref, dss.at[0], dsr.at[0], {"sub": other})

    def diag_to_band():
        arrive(dsib_ref, dss.at[0], dsr.at[0], {"sub": other})
        dsum_ref[...] = dsnd_ref[...] + dsib_ref[...]
        for k in range(1, nx):
            push(dsum_ref, drx_ref.at[k], dxs.at[k], dxr.at[k], {"cols": xpeer(k)})

    def diag_last():
        pivot_diag = dsum_ref[...]
        for k in range(1, nx):
            arrive(drx_ref.at[k], dxs.at[k], dxr.at[k], {"cols": xpeer(k)})
            pivot_diag = pivot_diag + drx_ref[k]
        scale = f32(1.0) / jnp.sqrt(pivot_diag)
        rs_ref[...] = jnp.transpose(jnp.broadcast_to(scale, (LANES, batch)))

    ket(0)
    multiply(0)
    x_step(0, 0)
    ket(1)
    multiply(1)
    x_step(1, 0)
    x_step(0, 1)
    ket(2)
    multiply(2)
    x_step(2, 0)
    x_step(1, 1)
    x_step(0, 2)
    ket(3)
    multiply(3)
    diag_to_sibling()
    x_step(3, 0)
    x_step(2, 1)
    x_step(1, 2)
    x_step(0, 3)
    diag_to_band()
    ket(4)
    x_step(3, 1)
    x_step(2, 2)
    x_step(1, 3)
    diag_last()
    finish(0)
    ket(5)
    x_step(3, 2)
    x_step(2, 3)
    finish(1)
    ket(6)
    x_step(3, 3)
    ket(7)
    finish(2)
    ket_last()
    finish(3)
    new_ref[...] = jnp.transpose(outt_ref[...]).astype(bf16)
    dout_ref[...] = diag_ref[...] - jnp.sum(squares[0], axis=0, keepdims=True)
    for copy in sends:
        copy.wait_send()


def body(
    nz,
    nx,
    stored_vectors,
    previous_columns,
    pivots,
    diagonal,
    ket_blocks,
    shell_tags,
    target_blocks,
    block_counts,
    shell_norms,
):
    depth, band = stored_vectors.shape
    rows_here, batch = previous_columns.shape
    slots, block_rows, _ = ket_blocks.shape
    blocks = rows_here // block_rows
    chunk = batch // nz
    grows = batch // PIVOT_GROUPS
    wide = -(-(depth + DIAG_PARTS) // LANES) * LANES
    zr, zl = nz // 2, nz - 1 - nz // 2
    half = nx // 2
    f32, bf16 = jnp.float32, jnp.bfloat16
    dma = pltpu.SemaphoreType.DMA
    vmem = pl.BlockSpec(memory_space=pltpu.VMEM)
    smem = pl.BlockSpec(memory_space=pltpu.SMEM)
    hbm = pl.BlockSpec(memory_space=pl.ANY)
    new_vectors, diag_out, next_columns = pl.pallas_call(
        functools.partial(kernel, nz, nx),
        out_shape=(
            jax.ShapeDtypeStruct((rows_here, batch), bf16),
            jax.ShapeDtypeStruct((1, rows_here), f32),
            jax.ShapeDtypeStruct((rows_here, batch), bf16),
        ),
        in_specs=[hbm, hbm, vmem, vmem, hbm, vmem, smem, smem, smem],
        out_specs=(vmem, vmem, vmem),
        scratch_shapes=[
            pltpu.VMEM((depth, band), bf16),
            pltpu.VMEM((rows_here, batch), bf16),
            pltpu.VMEM((slots, block_rows, batch), bf16),
            pltpu.VMEM((slots, block_rows, batch), bf16),
            pltpu.VMEM((batch, band), bf16),
            pltpu.VMEM((batch, wide), bf16),
            pltpu.VMEM((nz, chunk, wide), bf16),
            pltpu.VMEM((batch, wide), bf16),
            pltpu.VMEM((PIVOT_GROUPS, nx, grows, rows_here), f32),
            pltpu.VMEM((PIVOT_GROUPS, nx, grows, rows_here), f32),
            pltpu.VMEM((PIVOT_GROUPS, nx, grows, rows_here), f32),
            pltpu.VMEM((PIVOT_GROUPS, half, grows, rows_here), f32),
            pltpu.VMEM((PIVOT_GROUPS, half, grows, rows_here), f32),
            pltpu.VMEM((2, blocks, block_rows, batch), bf16),
            pltpu.VMEM((zr, blocks, block_rows, batch), bf16),
            pltpu.VMEM((zl, blocks, block_rows, batch), bf16),
            pltpu.VMEM((1, batch), f32),
            pltpu.VMEM((1, batch), f32),
            pltpu.VMEM((1, batch), f32),
            pltpu.VMEM((nx, 1, batch), f32),
            pltpu.VMEM((batch, rows_here), f32),
            pltpu.VMEM((batch, LANES), f32),
            pltpu.VMEM((batch, rows_here), f32),
            dma((4,)),
            dma((2,)),
            dma((nz,)),
            dma((nz,)),
            dma((nz,)),
            dma((nz,)),
            dma((PIVOT_GROUPS, half)),
            dma((PIVOT_GROUPS, half)),
            dma((PIVOT_GROUPS, half)),
            dma((PIVOT_GROUPS, half)),
            dma((PIVOT_GROUPS, half)),
            dma((PIVOT_GROUPS, half)),
            dma((zr, blocks)),
            dma((zr, blocks)),
            dma((zl, blocks)),
            dma((zl, blocks)),
            dma((1,)),
            dma((1,)),
            dma((nx,)),
            dma((nx,)),
        ],
        compiler_params=pltpu.CompilerParams(
            collective_id=0, has_side_effects=True, vmem_limit_bytes=48 * 1024 * 1024
        ),
        name="downdate",
    )(
        stored_vectors,
        previous_columns,
        pivots.reshape(1, batch),
        diagonal.reshape(1, rows_here),
        ket_blocks,
        shell_tags,
        target_blocks.T,
        block_counts,
        shell_norms,
    )
    return new_vectors, diag_out.reshape(rows_here), next_columns


def solution(mesh):
    return jax.shard_map(
        functools.partial(body, mesh.shape["rows"], mesh.shape["cols"]),
        mesh=mesh,
        in_specs=(
            P(("cols", "sub"), ("groups", "rows")),
            P(("groups", "rows", "cols", "sub"), None),
            P("groups"),
            P(("groups", "rows", "cols", "sub")),
            P(("groups", "rows", "cols", "sub"), None, None),
            P(("groups", "rows", "cols", "sub"), None),
            P("groups", None),
            P("groups"),
            P(),
        ),
        out_specs=(
            P(("groups", "rows", "cols", "sub"), None),
            P(("groups", "rows", "cols", "sub")),
            P(("groups", "rows", "cols", "sub"), None),
        ),
        check_vma=False,
    )
```

```python
import functools

import jax
import jax.numpy as jnp
from jax import lax
from jax.experimental import pallas as pl
from jax.experimental.pallas import tpu as pltpu
from jax.sharding import PartitionSpec as P

MESH = pl.DeviceIdType.MESH
LANES = 128
PIVOT_GROUPS = 4
DIAG_PARTS = 3
BEFORE = 2


def kernel(
    nz,
    nx,
    v_hbm,
    prev_hbm,
    piv_hbm,
    diag_hbm,
    ket_hbm,
    tags_hbm,
    tgt_hbm,
    cnt_hbm,
    norms_hbm,
    new_hbm,
    dout_hbm,
    next_hbm,
    new_ref,
    dout_ref,
    next_ref,
    piv_ref,
    diag_ref,
    tags_ref,
    tgt_ref,
    cnt_ref,
    norms_ref,
    v_ref,
    prev_ref,
    ket_ref,
    fresh_ref,
    hot_ref,
    pick_ref,
    rx1_ref,
    pful_ref,
    snd_ref,
    loc_ref,
    rsib_ref,
    rxr_ref,
    rxl_ref,
    k0_ref,
    krr_ref,
    krl_ref,
    dsnd_ref,
    dsib_ref,
    dsum_ref,
    drx_ref,
    prevt_ref,
    rs_ref,
    outt_ref,
    vsem,
    lsem,
    p1s,
    p1r,
    p2s,
    p2r,
    d2s,
    d2r,
    xrs,
    xrr,
    xls,
    xlr,
    krs,
    krq,
    kls,
    klq,
    dss,
    dsr,
    dxs,
    dxr,
    osem,
):
    f32, bf16 = jnp.float32, jnp.bfloat16
    depth, band = v_ref.shape
    rows_here, batch = prev_ref.shape
    slots, block_rows = ket_ref.shape[0], ket_ref.shape[1]
    blocks = rows_here // block_rows
    chunk = batch // nz
    per = nz // PIVOT_GROUPS
    grows = per * chunk
    half = nx // 2
    r, c, s = lax.axis_index("rows"), lax.axis_index("cols"), lax.axis_index("sub")
    other = 1 - s
    device = (r * nx + c) * 2 + s
    right, left = lax.rem(c + 1, nx), lax.rem(c + nx - 1, nx)
    up, down = lax.rem(r + 1, nz), lax.rem(r + nz - 1, nz)

    def zpeer(k):
        return lax.rem(r + k, nz)

    def xpeer(k):
        return lax.rem(c + k, nx)

    smalls = [
        pltpu.make_async_copy(src, dst, lsem.at[2 + i])
        for i, (src, dst) in enumerate(
            (
                (piv_hbm, piv_ref),
                (diag_hbm, diag_ref),
                (tags_hbm, tags_ref),
                (tgt_hbm, tgt_ref),
                (cnt_hbm, cnt_ref),
                (norms_hbm, norms_ref),
            )
        )
    ]
    for copy in smalls:
        copy.start()
    pieces = 4
    width = band // pieces
    vload = [
        pltpu.make_async_copy(
            v_hbm.at[:, pl.ds(i * width, width)], v_ref.at[:, pl.ds(i * width, width)], vsem.at[i]
        )
        for i in range(pieces)
    ]
    for copy in vload:
        copy.start()
    ketload = pltpu.make_async_copy(ket_hbm, ket_ref, lsem.at[0])
    ketload.start()
    prevload = pltpu.make_async_copy(prev_hbm, prev_ref, lsem.at[1])
    prevload.start()

    barrier = pltpu.get_barrier_semaphore()
    by_reach = sorted(range(1, nz), key=lambda k: -min(k, nz - k))
    for k in by_reach:
        pl.semaphore_signal(barrier, inc=1, device_id={"rows": zpeer(k)}, device_id_type=MESH)
    for k in range(1, nx):
        pl.semaphore_signal(barrier, inc=1, device_id={"cols": xpeer(k)}, device_id_type=MESH)
    pl.semaphore_signal(barrier, inc=1, device_id={"sub": other}, device_id_type=MESH)

    for copy in smalls[:2]:
        copy.wait()
    pivot_cols = jnp.transpose(jnp.broadcast_to(piv_ref[...], (LANES, batch)))
    lane = lax.broadcasted_iota(jnp.int32, (batch, LANES), 1)
    in_band = pivot_cols - r * band - lane
    for t in range(band // LANES):
        hot = jnp.where(in_band == t * LANES, f32(1.0), f32(0.0)).astype(bf16)
        hot_ref[:, t * LANES : (t + 1) * LANES] = hot
    in_device = pivot_cols - device * rows_here - lane
    found = jnp.zeros((batch, LANES), f32)
    for t in range(rows_here // LANES):
        row = diag_ref[:, t * LANES : (t + 1) * LANES]
        found = found + jnp.where(in_device == t * LANES, row, f32(0.0))
    own_diag = jnp.sum(found, axis=1, keepdims=True)
    part_hi = own_diag.astype(bf16).astype(f32)
    part_mid = (own_diag - part_hi).astype(bf16).astype(f32)
    part_lo = own_diag - part_hi - part_mid
    spare = pick_ref.shape[1] - depth
    place = lax.broadcasted_iota(jnp.int32, (batch, spare), 1)
    extra = jnp.where(place == 0, part_hi, f32(0.0))
    extra = jnp.where(place == 1, part_mid, extra)
    extra = jnp.where(place == 2, part_lo, extra)
    pick_ref[:, depth:] = extra.astype(bf16)
    picked = jnp.zeros((batch, depth), f32)
    for i in range(pieces):
        vload[i].wait()
        span = slice(i * width, (i + 1) * width)
        picked = picked + lax.dot_general(
            hot_ref[:, span], v_ref[:, span], (((1,), (1,)), ((), ())), preferred_element_type=f32
        )
    pick_ref[:, :depth] = picked.astype(bf16)

    pl.semaphore_wait(barrier, nz - 1 + nx - 1 + 1)

    def push(src, dst, send_sem, recv_sem, to):
        copy = pltpu.make_async_remote_copy(
            src_ref=src,
            dst_ref=dst,
            send_sem=send_sem,
            recv_sem=recv_sem,
            device_id=to,
            device_id_type=MESH,
        )
        copy.start()

    def tally(ref, sem, to, sent=False):
        copy = pltpu.make_async_remote_copy(
            src_ref=ref,
            dst_ref=ref,
            send_sem=sem,
            recv_sem=sem,
            device_id=to,
            device_id_type=MESH,
        )
        if sent:
            copy.wait_send()
        else:
            copy.wait_recv()

    for k in by_reach:
        to = zpeer(k)
        start = pl.multiple_of(to * chunk, chunk)
        push(
            pick_ref.at[pl.ds(start, chunk), :], rx1_ref.at[k - 1], p1s.at[0], p1r.at[0], {"rows": to}
        )

    ketload.wait()
    for copy in smalls[2:]:
        copy.wait()
    tags = tags_ref[...]
    factor = jnp.zeros(tags.shape, f32)
    for kind in range(norms_ref.shape[0]):
        factor = jnp.where(tags == kind, norms_ref[kind], factor)
    for t in range(slots):
        column = jnp.transpose(jnp.broadcast_to(factor[t : t + 1, :], (LANES, block_rows)))
        for h in range(batch // LANES):
            span = slice(h * LANES, (h + 1) * LANES)
            fresh_ref[t, :, span] = (ket_ref[t, :, span].astype(f32) * column).astype(bf16)
    prevload.wait()
    prevt_ref[...] = jnp.transpose(prev_ref[...].astype(f32))

    targets = [jnp.where(t < cnt_ref[device], tgt_ref[t, device], -1) for t in range(slots)]

    def with_own(value, reach, w):
        block = ((lax.rem(r + reach + nz, nz) * nx + c) * 2 + s) * blocks + w
        for t in range(slots):
            value = jnp.where(targets[t] == block, fresh_ref[t], value)
        return value

    zr, zl = nz // 2, nz - 1 - nz // 2

    def ket_right(i):
        if i >= zr:
            return
        for w in range(blocks):
            if i == 0:
                src = k0_ref.at[0, w]
                src[...] = with_own(jnp.zeros(fresh_ref.shape[1:], bf16), zr, w)
            else:
                src = krr_ref.at[i - 1, w]
                tally(src, krq.at[i - 1, w], {"rows": up})
                src[...] = with_own(src[...], zr - i, w)
            push(src, krr_ref.at[i, w], krs.at[0], krq.at[i, w], {"rows": up})

    def ket_left(i):
        if i >= zl:
            return
        for w in range(blocks):
            if i == 0:
                src = k0_ref.at[1, w]
                src[...] = with_own(jnp.zeros(fresh_ref.shape[1:], bf16), -zl, w)
            else:
                src = krl_ref.at[i - 1, w]
                tally(src, klq.at[i - 1, w], {"rows": down})
                src[...] = with_own(src[...], i - zl, w)
            push(src, krl_ref.at[i, w], kls.at[0], klq.at[i, w], {"rows": down})

    def ket(i):
        ket_right(i)
        ket_left(i)

    def ket_last():
        for w in range(blocks):
            tally(krr_ref.at[zr - 1, w], krq.at[zr - 1, w], {"rows": up})
            tally(krl_ref.at[zl - 1, w], klq.at[zl - 1, w], {"rows": down})
            both = krr_ref[zr - 1, w].astype(f32) + krl_ref[zl - 1, w].astype(f32)
            next_ref[w * block_rows : (w + 1) * block_rows, :] = with_own(both.astype(bf16), 0, w)

    ket(0)

    def broadcast():
        for k in reversed(by_reach):
            at = ((BEFORE - k) % nz) * chunk
            push(
                pful_ref.at[mine, :],
                pful_ref.at[pl.ds(at, chunk), :],
                p2s.at[0],
                p2r.at[((BEFORE - k) % nz) // per],
                {"rows": zpeer(k)},
            )

    mine = slice(BEFORE * chunk, (BEFORE + 1) * chunk)

    own = pl.multiple_of(r * chunk, chunk)
    total = pick_ref[pl.ds(own, chunk), :].astype(f32)
    tally(rx1_ref, p1r.at[0], {"rows": up})
    for k in range(1, nz):
        total = total + rx1_ref[k - 1].astype(f32)
    pful_ref[mine, :] = total.astype(bf16)
    broadcast()
    order = [(half - p // 2) if p % 2 == 0 else (half + (p + 1) // 2) % nx for p in range(nx)]
    where_is = {rel: p for p, rel in enumerate(order)}
    members = [0, 1, PIVOT_GROUPS - 1] + list(range(2, PIVOT_GROUPS - 1))
    pairs = nx // 2

    def columns_of(p, core):
        rel = order[p]
        return pl.multiple_of((xpeer(rel) * 2 + core) * rows_here, rows_here)

    def multiply(g):
        first = members[g] * per
        coming = per - (1 if first <= BEFORE < first + per else 0)
        tally(pful_ref.at[pl.ds(0, coming * chunk), :], p2r.at[members[g]], {"rows": up})
        lhs = pful_ref[first * chunk : first * chunk + grows, :depth]
        for m in range(pairs):
            for p in (2 * m, 2 * m + 1):
                snd_ref[g, p] = jnp.dot(
                    lhs, v_ref[:, pl.ds(columns_of(p, other), rows_here)], preferred_element_type=f32
                )
            span = pl.ds(2 * m, 2)
            push(
                snd_ref.at[g, span], rsib_ref.at[g, span], d2s.at[0], d2r.at[g, m], {"sub": other}
            )
        for p in range(nx):
            loc_ref[g, p] = jnp.dot(
                lhs, v_ref[:, pl.ds(columns_of(p, s), rows_here)], preferred_element_type=f32
            )

    met = set()

    def chip_part(g, p):
        m = p // 2
        if (g, m) not in met:
            met.add((g, m))
            tally(rsib_ref.at[g, pl.ds(2 * m, 2)], d2r.at[g, m], {"sub": other})
        return loc_ref[g, p] + rsib_ref[g, p]

    def hops(g):
        longer = list(range(half, 0, -1)), list(range(nx - half + 1, nx))
        shorter = list(range(half - 1, 0, -1)), list(range(nx - half, nx))
        return longer if g % 2 == 0 else shorter

    def spot(g, way, i):
        return sum(len(hops(q)[way]) for q in range(g)) + i

    def x_step(g, i):
        for way, (buf, ss, rs, to) in enumerate(
            ((rxr_ref, xrs, xrr, right), (rxl_ref, xls, xlr, left))
        ):
            path = hops(g)[way]
            if i >= len(path):
                continue
            p = where_is[path[i]]
            value = chip_part(g, p)
            if i > 0:
                came = spot(g, way, i - 1)
                tally(buf.at[came], rs.at[came], {"cols": to})
                value = value + buf[came]
            loc_ref[g, p] = value
            goes = spot(g, way, i)
            push(loc_ref.at[g, p], buf.at[goes], ss.at[0], rs.at[goes], {"cols": to})

    squares = [jnp.zeros((chunk, rows_here), f32)]

    def finish(g):
        value = chip_part(g, where_is[0])
        for way, (buf, ss, rs, to) in enumerate(
            ((rxr_ref, xrs, xrr, right), (rxl_ref, xls, xlr, left))
        ):
            last = spot(g, way, len(hops(g)[way]) - 1)
            tally(buf.at[last], rs.at[last], {"cols": to})
            value = value + buf[last]
        for q in range(per):
            p = members[g] * per + q
            at = pl.multiple_of(lax.rem(p + r + nz - BEFORE, nz) * chunk, chunk)
            scale = rs_ref[p * chunk : (p + 1) * chunk, :]
            scale = jnp.concatenate([scale] * (rows_here // LANES), axis=1)
            scaled = (prevt_ref[pl.ds(at, chunk), :] - value[q * chunk : (q + 1) * chunk]) * scale
            squares[0] = squares[0] + scaled * scaled
            outt_ref[pl.ds(at, chunk), :] = scaled

    def diag_to_sibling():
        tile = depth // LANES
        at = depth - tile * LANES
        turned = jnp.transpose(pful_ref[:, tile * LANES : (tile + 1) * LANES].astype(f32))
        dsnd_ref[...] = (
            turned[at : at + 1, :] + turned[at + 1 : at + 2, :] + turned[at + 2 : at + 3, :]
        )
        push(dsnd_ref, dsib_ref, dss.at[0], dsr.at[0], {"sub": other})

    def diag_to_band():
        tally(dsib_ref, dsr.at[0], {"sub": other})
        dsum_ref[...] = dsnd_ref[...] + dsib_ref[...]
        for k in range(1, nx):
            push(dsum_ref, drx_ref.at[k - 1], dxs.at[0], dxr.at[0], {"cols": xpeer(k)})

    def diag_last():
        pivot_diag = dsum_ref[...]
        tally(drx_ref, dxr.at[0], {"cols": right})
        for k in range(1, nx):
            pivot_diag = pivot_diag + drx_ref[k - 1]
        scale = f32(1.0) / jnp.sqrt(pivot_diag)
        rs_ref[...] = jnp.transpose(jnp.broadcast_to(scale, (LANES, batch)))

    ket(1)
    multiply(0)
    x_step(0, 0)
    multiply(1)
    x_step(1, 0)
    ket(2)
    x_step(0, 1)
    multiply(2)
    x_step(2, 0)
    x_step(1, 1)
    ket(3)
    x_step(0, 2)
    multiply(3)
    diag_to_sibling()
    x_step(3, 0)
    x_step(2, 1)
    ket(4)
    x_step(1, 2)
    x_step(0, 3)
    diag_to_band()
    x_step(3, 1)
    x_step(2, 2)
    ket(5)
    x_step(1, 3)
    diag_last()
    finish(0)
    x_step(3, 2)
    x_step(2, 3)
    ket(6)
    finish(1)
    x_step(3, 3)
    ket(7)
    finish(2)
    ket_last()
    finish(3)
    new_ref[...] = jnp.transpose(outt_ref[...]).astype(bf16)
    dout_ref[...] = diag_ref[...] - jnp.sum(squares[0], axis=0, keepdims=True)
    outs = [
        pltpu.make_async_copy(src, dst, osem.at[i])
        for i, (src, dst) in enumerate(
            ((new_ref, new_hbm), (dout_ref, dout_hbm), (next_ref, next_hbm))
        )
    ]
    for copy in outs:
        copy.start()
    for ref, sem, to in (
        (rx1_ref, p1s, {"rows": up}),
        (rx1_ref, p2s, {"rows": up}),
        (rsib_ref, d2s, {"sub": other}),
        (rxr_ref, xrs, {"cols": right}),
        (rxl_ref, xls, {"cols": left}),
        (krr_ref, krs, {"rows": up}),
        (krl_ref, kls, {"rows": down}),
        (dsib_ref, dss, {"sub": other}),
        (drx_ref, dxs, {"cols": right}),
    ):
        tally(ref, sem.at[0], to, sent=True)
    for copy in outs:
        copy.wait()


def body(
    nz,
    nx,
    stored_vectors,
    previous_columns,
    pivots,
    diagonal,
    ket_blocks,
    shell_tags,
    target_blocks,
    block_counts,
    shell_norms,
):
    depth, band = stored_vectors.shape
    rows_here, batch = previous_columns.shape
    slots, block_rows, _ = ket_blocks.shape
    blocks = rows_here // block_rows
    chunk = batch // nz
    grows = batch // PIVOT_GROUPS
    wide = -(-(depth + DIAG_PARTS) // LANES) * LANES
    zr, zl = nz // 2, nz - 1 - nz // 2
    half = nx // 2
    x_messages = PIVOT_GROUPS * (nx - 1) // 2
    f32, bf16 = jnp.float32, jnp.bfloat16
    dma = pltpu.SemaphoreType.DMA
    vmem = pl.BlockSpec(memory_space=pltpu.VMEM)
    hbm = pl.BlockSpec(memory_space=pltpu.HBM)
    new_vectors, diag_out, next_columns = pl.pallas_call(
        functools.partial(kernel, nz, nx),
        out_shape=(
            jax.ShapeDtypeStruct((rows_here, batch), bf16),
            jax.ShapeDtypeStruct((1, rows_here), f32),
            jax.ShapeDtypeStruct((rows_here, batch), bf16),
        ),
        in_specs=[hbm] * 9,
        out_specs=(hbm, hbm, hbm),
        scratch_shapes=[
            pltpu.VMEM((rows_here, batch), bf16),
            pltpu.VMEM((1, rows_here), f32),
            pltpu.VMEM((rows_here, batch), bf16),
            pltpu.VMEM((1, batch), jnp.int32),
            pltpu.VMEM((1, rows_here), f32),
            pltpu.VMEM((slots, block_rows), jnp.int32),
            pltpu.SMEM(target_blocks.shape[::-1], jnp.int32),
            pltpu.SMEM(block_counts.shape, jnp.int32),
            pltpu.SMEM(shell_norms.shape, f32),
            pltpu.VMEM((depth, band), bf16),
            pltpu.VMEM((rows_here, batch), bf16),
            pltpu.VMEM((slots, block_rows, batch), bf16),
            pltpu.VMEM((slots, block_rows, batch), bf16),
            pltpu.VMEM((batch, band), bf16),
            pltpu.VMEM((batch, wide), bf16),
            pltpu.VMEM((nz - 1, chunk, wide), bf16),
            pltpu.VMEM((batch, wide), bf16),
            pltpu.VMEM((PIVOT_GROUPS, nx, grows, rows_here), f32),
            pltpu.VMEM((PIVOT_GROUPS, nx, grows, rows_here), f32),
            pltpu.VMEM((PIVOT_GROUPS, nx, grows, rows_here), f32),
            pltpu.VMEM((x_messages, grows, rows_here), f32),
            pltpu.VMEM((x_messages, grows, rows_here), f32),
            pltpu.VMEM((2, blocks, block_rows, batch), bf16),
            pltpu.VMEM((zr, blocks, block_rows, batch), bf16),
            pltpu.VMEM((zl, blocks, block_rows, batch), bf16),
            pltpu.VMEM((1, batch), f32),
            pltpu.VMEM((1, batch), f32),
            pltpu.VMEM((1, batch), f32),
            pltpu.VMEM((nx - 1, 1, batch), f32),
            pltpu.VMEM((batch, rows_here), f32),
            pltpu.VMEM((batch, LANES), f32),
            pltpu.VMEM((batch, rows_here), f32),
            dma((4,)),
            dma((8,)),
            dma((1,)),
            dma((1,)),
            dma((1,)),
            dma((PIVOT_GROUPS,)),
            dma((1,)),
            dma((PIVOT_GROUPS, half)),
            dma((1,)),
            dma((x_messages,)),
            dma((1,)),
            dma((x_messages,)),
            dma((1,)),
            dma((zr, blocks)),
            dma((1,)),
            dma((zl, blocks)),
            dma((1,)),
            dma((1,)),
            dma((1,)),
            dma((1,)),
            dma((3,)),
        ],
        compiler_params=pltpu.CompilerParams(
            collective_id=0, has_side_effects=True, vmem_limit_bytes=67043328
        ),
        name="downdate",
    )(
        stored_vectors,
        previous_columns,
        pivots.reshape(1, batch),
        diagonal.reshape(1, rows_here),
        ket_blocks,
        shell_tags,
        target_blocks.T,
        block_counts,
        shell_norms,
    )
    return new_vectors, diag_out.reshape(rows_here), next_columns


def solution(mesh):
    return jax.shard_map(
        functools.partial(body, mesh.shape["rows"], mesh.shape["cols"]),
        mesh=mesh,
        in_specs=(
            P(("cols", "sub"), ("groups", "rows")),
            P(("groups", "rows", "cols", "sub"), None),
            P("groups"),
            P(("groups", "rows", "cols", "sub")),
            P(("groups", "rows", "cols", "sub"), None, None),
            P(("groups", "rows", "cols", "sub"), None),
            P("groups", None),
            P("groups"),
            P(),
        ),
        out_specs=(
            P(("groups", "rows", "cols", "sub"), None),
            P(("groups", "rows", "cols", "sub")),
            P(("groups", "rows", "cols", "sub"), None),
        ),
        check_vma=False,
    )
```

```python
import functools

import jax
import jax.numpy as jnp
from jax import lax
from jax.experimental import pallas as pl
from jax.experimental.pallas import tpu as pltpu
from jax.sharding import PartitionSpec as P

MESH = pl.DeviceIdType.MESH
LANES = 128
PIVOT_GROUPS = 4
DIAG_PARTS = 3
BEFORE = 2


def kernel(
    nz,
    nx,
    v_hbm,
    prev_hbm,
    piv_hbm,
    diag_hbm,
    ket_hbm,
    tags_hbm,
    tgt_hbm,
    cnt_hbm,
    norms_hbm,
    new_ref,
    dout_ref,
    next_ref,
    piv_ref,
    diag_ref,
    tags_ref,
    tgt_ref,
    cnt_ref,
    norms_ref,
    v_ref,
    prev_ref,
    ket_ref,
    fresh_ref,
    hot_ref,
    pick_ref,
    rx1_ref,
    pful_ref,
    snd_ref,
    loc_ref,
    rsib_ref,
    rxr_ref,
    rxl_ref,
    k0_ref,
    krr_ref,
    krl_ref,
    dsnd_ref,
    dsib_ref,
    dsum_ref,
    drx_ref,
    prevt_ref,
    rs_ref,
    outt_ref,
    vsem,
    lsem,
    p1s,
    p1r,
    p2s,
    p2r,
    d2s,
    d2r,
    xrs,
    xrr,
    xls,
    xlr,
    krs,
    krq,
    kls,
    klq,
    dss,
    dsr,
    dxs,
    dxr,
):
    f32, bf16 = jnp.float32, jnp.bfloat16
    depth, band = v_ref.shape
    rows_here, batch = prev_ref.shape
    slots, block_rows = ket_ref.shape[0], ket_ref.shape[1]
    blocks = rows_here // block_rows
    chunk = batch // nz
    per = nz // PIVOT_GROUPS
    grows = per * chunk
    half = nx // 2
    r, c, s = lax.axis_index("rows"), lax.axis_index("cols"), lax.axis_index("sub")
    other = 1 - s
    device = (r * nx + c) * 2 + s
    right, left = lax.rem(c + 1, nx), lax.rem(c + nx - 1, nx)
    up, down = lax.rem(r + 1, nz), lax.rem(r + nz - 1, nz)

    def zpeer(k):
        return lax.rem(r + k, nz)

    def xpeer(k):
        return lax.rem(c + k, nx)

    smalls = [
        pltpu.make_async_copy(src, dst, lsem.at[2 + i])
        for i, (src, dst) in enumerate(
            (
                (piv_hbm, piv_ref),
                (diag_hbm, diag_ref),
                (tags_hbm, tags_ref),
                (tgt_hbm, tgt_ref),
                (cnt_hbm, cnt_ref),
                (norms_hbm, norms_ref),
            )
        )
    ]
    for copy in smalls:
        copy.start()
    pieces = 4
    width = band // pieces
    vload = [
        pltpu.make_async_copy(
            v_hbm.at[:, pl.ds(i * width, width)], v_ref.at[:, pl.ds(i * width, width)], vsem.at[i]
        )
        for i in range(pieces)
    ]
    for copy in vload:
        copy.start()
    ketload = pltpu.make_async_copy(ket_hbm, ket_ref, lsem.at[0])
    ketload.start()
    prevload = pltpu.make_async_copy(prev_hbm, prev_ref, lsem.at[1])
    prevload.start()

    barrier = pltpu.get_barrier_semaphore()
    by_reach = sorted(range(1, nz), key=lambda k: -min(k, nz - k))
    for k in by_reach:
        pl.semaphore_signal(barrier, inc=1, device_id={"rows": zpeer(k)}, device_id_type=MESH)
    for k in range(1, nx):
        pl.semaphore_signal(barrier, inc=1, device_id={"cols": xpeer(k)}, device_id_type=MESH)
    pl.semaphore_signal(barrier, inc=1, device_id={"sub": other}, device_id_type=MESH)

    for copy in smalls[:2]:
        copy.wait()
    pivot_cols = jnp.transpose(jnp.broadcast_to(piv_ref[...], (LANES, batch)))
    lane = lax.broadcasted_iota(jnp.int32, (batch, LANES), 1)
    in_band = pivot_cols - r * band - lane
    for t in range(band // LANES):
        hot = jnp.where(in_band == t * LANES, f32(1.0), f32(0.0)).astype(bf16)
        hot_ref[:, t * LANES : (t + 1) * LANES] = hot
    in_device = pivot_cols - device * rows_here - lane
    found = jnp.zeros((batch, LANES), f32)
    for t in range(rows_here // LANES):
        row = diag_ref[:, t * LANES : (t + 1) * LANES]
        found = found + jnp.where(in_device == t * LANES, row, f32(0.0))
    own_diag = jnp.sum(found, axis=1, keepdims=True)
    part_hi = own_diag.astype(bf16).astype(f32)
    part_mid = (own_diag - part_hi).astype(bf16).astype(f32)
    part_lo = own_diag - part_hi - part_mid
    spare = pick_ref.shape[1] - depth
    place = lax.broadcasted_iota(jnp.int32, (batch, spare), 1)
    extra = jnp.where(place == 0, part_hi, f32(0.0))
    extra = jnp.where(place == 1, part_mid, extra)
    extra = jnp.where(place == 2, part_lo, extra)
    pick_ref[:, depth:] = extra.astype(bf16)
    picked = jnp.zeros((batch, depth), f32)
    for i in range(pieces):
        vload[i].wait()
        span = slice(i * width, (i + 1) * width)
        picked = picked + lax.dot_general(
            hot_ref[:, span], v_ref[:, span], (((1,), (1,)), ((), ())), preferred_element_type=f32
        )
    pick_ref[:, :depth] = picked.astype(bf16)

    pl.semaphore_wait(barrier, nz - 1 + nx - 1 + 1)

    def push(src, dst, send_sem, recv_sem, to):
        copy = pltpu.make_async_remote_copy(
            src_ref=src,
            dst_ref=dst,
            send_sem=send_sem,
            recv_sem=recv_sem,
            device_id=to,
            device_id_type=MESH,
        )
        copy.start()

    def tally(ref, sem, to, sent=False):
        copy = pltpu.make_async_remote_copy(
            src_ref=ref,
            dst_ref=ref,
            send_sem=sem,
            recv_sem=sem,
            device_id=to,
            device_id_type=MESH,
        )
        if sent:
            copy.wait_send()
        else:
            copy.wait_recv()

    for k in by_reach:
        to = zpeer(k)
        start = pl.multiple_of(to * chunk, chunk)
        push(
            pick_ref.at[pl.ds(start, chunk), :], rx1_ref.at[k - 1], p1s.at[0], p1r.at[0], {"rows": to}
        )

    ketload.wait()
    for copy in smalls[2:]:
        copy.wait()
    tags = tags_ref[...]
    factor = jnp.zeros(tags.shape, f32)
    for kind in range(norms_ref.shape[0]):
        factor = jnp.where(tags == kind, norms_ref[kind], factor)
    for t in range(slots):
        column = jnp.transpose(jnp.broadcast_to(factor[t : t + 1, :], (LANES, block_rows)))
        for h in range(batch // LANES):
            span = slice(h * LANES, (h + 1) * LANES)
            fresh_ref[t, :, span] = (ket_ref[t, :, span].astype(f32) * column).astype(bf16)
    prevload.wait()
    prevt_ref[...] = jnp.transpose(prev_ref[...].astype(f32))

    targets = [jnp.where(t < cnt_ref[device], tgt_ref[t, device], -1) for t in range(slots)]

    def with_own(value, reach, w):
        block = ((lax.rem(r + reach + nz, nz) * nx + c) * 2 + s) * blocks + w
        for t in range(slots):
            value = jnp.where(targets[t] == block, fresh_ref[t], value)
        return value

    zr, zl = nz // 2, nz - 1 - nz // 2

    def ket_right(i):
        if i >= zr:
            return
        for w in range(blocks):
            if i == 0:
                src = k0_ref.at[0, w]
                src[...] = with_own(jnp.zeros(fresh_ref.shape[1:], bf16), zr, w)
            else:
                src = krr_ref.at[i - 1, w]
                tally(src, krq.at[i - 1, w], {"rows": up})
                src[...] = with_own(src[...], zr - i, w)
            push(src, krr_ref.at[i, w], krs.at[0], krq.at[i, w], {"rows": up})

    def ket_left(i):
        if i >= zl:
            return
        for w in range(blocks):
            if i == 0:
                src = k0_ref.at[1, w]
                src[...] = with_own(jnp.zeros(fresh_ref.shape[1:], bf16), -zl, w)
            else:
                src = krl_ref.at[i - 1, w]
                tally(src, klq.at[i - 1, w], {"rows": down})
                src[...] = with_own(src[...], i - zl, w)
            push(src, krl_ref.at[i, w], kls.at[0], klq.at[i, w], {"rows": down})

    def ket(i):
        ket_right(i)
        ket_left(i)

    def ket_last():
        for w in range(blocks):
            tally(krr_ref.at[zr - 1, w], krq.at[zr - 1, w], {"rows": up})
            tally(krl_ref.at[zl - 1, w], klq.at[zl - 1, w], {"rows": down})
            both = krr_ref[zr - 1, w].astype(f32) + krl_ref[zl - 1, w].astype(f32)
            next_ref[w * block_rows : (w + 1) * block_rows, :] = with_own(both.astype(bf16), 0, w)

    ket(0)

    def broadcast():
        for k in reversed(by_reach):
            at = ((BEFORE - k) % nz) * chunk
            push(
                pful_ref.at[mine, :],
                pful_ref.at[pl.ds(at, chunk), :],
                p2s.at[0],
                p2r.at[((BEFORE - k) % nz) // per],
                {"rows": zpeer(k)},
            )

    mine = slice(BEFORE * chunk, (BEFORE + 1) * chunk)

    own = pl.multiple_of(r * chunk, chunk)
    total = pick_ref[pl.ds(own, chunk), :].astype(f32)
    tally(rx1_ref, p1r.at[0], {"rows": up})
    for k in range(1, nz):
        total = total + rx1_ref[k - 1].astype(f32)
    pful_ref[mine, :] = total.astype(bf16)
    broadcast()
    order = [(half - p // 2) if p % 2 == 0 else (half + (p + 1) // 2) % nx for p in range(nx)]
    where_is = {rel: p for p, rel in enumerate(order)}
    members = [0, 1, PIVOT_GROUPS - 1] + list(range(2, PIVOT_GROUPS - 1))
    pairs = nx // 2

    def columns_of(p, core):
        rel = order[p]
        return pl.multiple_of((xpeer(rel) * 2 + core) * rows_here, rows_here)

    def multiply(g):
        first = members[g] * per
        coming = per - (1 if first <= BEFORE < first + per else 0)
        tally(pful_ref.at[pl.ds(0, coming * chunk), :], p2r.at[members[g]], {"rows": up})
        lhs = pful_ref[first * chunk : first * chunk + grows, :depth]
        for m in range(pairs):
            for p in (2 * m, 2 * m + 1):
                snd_ref[g, p] = jnp.dot(
                    lhs, v_ref[:, pl.ds(columns_of(p, other), rows_here)], preferred_element_type=f32
                )
            span = pl.ds(2 * m, 2)
            push(
                snd_ref.at[g, span], rsib_ref.at[g, span], d2s.at[0], d2r.at[g, m], {"sub": other}
            )
        for p in range(nx):
            loc_ref[g, p] = jnp.dot(
                lhs, v_ref[:, pl.ds(columns_of(p, s), rows_here)], preferred_element_type=f32
            )

    met = set()

    def chip_part(g, p):
        m = p // 2
        if (g, m) not in met:
            met.add((g, m))
            tally(rsib_ref.at[g, pl.ds(2 * m, 2)], d2r.at[g, m], {"sub": other})
        return loc_ref[g, p] + rsib_ref[g, p]

    def hops(g):
        longer = list(range(half, 0, -1)), list(range(nx - half + 1, nx))
        shorter = list(range(half - 1, 0, -1)), list(range(nx - half, nx))
        return longer if g % 2 == 0 else shorter

    def spot(g, way, i):
        return sum(len(hops(q)[way]) for q in range(g)) + i

    def x_step(g, i):
        for way, (buf, ss, rs, to) in enumerate(
            ((rxr_ref, xrs, xrr, right), (rxl_ref, xls, xlr, left))
        ):
            path = hops(g)[way]
            if i >= len(path):
                continue
            p = where_is[path[i]]
            value = chip_part(g, p)
            if i > 0:
                came = spot(g, way, i - 1)
                tally(buf.at[came], rs.at[came], {"cols": to})
                value = value + buf[came]
            loc_ref[g, p] = value
            goes = spot(g, way, i)
            push(loc_ref.at[g, p], buf.at[goes], ss.at[0], rs.at[goes], {"cols": to})

    squares = [jnp.zeros((chunk, rows_here), f32)]

    def finish(g):
        value = chip_part(g, where_is[0])
        for way, (buf, ss, rs, to) in enumerate(
            ((rxr_ref, xrs, xrr, right), (rxl_ref, xls, xlr, left))
        ):
            last = spot(g, way, len(hops(g)[way]) - 1)
            tally(buf.at[last], rs.at[last], {"cols": to})
            value = value + buf[last]
        for q in range(per):
            p = members[g] * per + q
            at = pl.multiple_of(lax.rem(p + r + nz - BEFORE, nz) * chunk, chunk)
            scale = rs_ref[p * chunk : (p + 1) * chunk, :]
            scale = jnp.concatenate([scale] * (rows_here // LANES), axis=1)
            scaled = (prevt_ref[pl.ds(at, chunk), :] - value[q * chunk : (q + 1) * chunk]) * scale
            squares[0] = squares[0] + scaled * scaled
            outt_ref[pl.ds(at, chunk), :] = scaled

    def diag_to_sibling():
        tile = depth // LANES
        at = depth - tile * LANES
        turned = jnp.transpose(pful_ref[:, tile * LANES : (tile + 1) * LANES].astype(f32))
        dsnd_ref[...] = (
            turned[at : at + 1, :] + turned[at + 1 : at + 2, :] + turned[at + 2 : at + 3, :]
        )
        push(dsnd_ref, dsib_ref, dss.at[0], dsr.at[0], {"sub": other})

    def diag_to_band():
        tally(dsib_ref, dsr.at[0], {"sub": other})
        dsum_ref[...] = dsnd_ref[...] + dsib_ref[...]
        for k in range(1, nx):
            push(dsum_ref, drx_ref.at[k - 1], dxs.at[0], dxr.at[0], {"cols": xpeer(k)})

    def diag_last():
        pivot_diag = dsum_ref[...]
        tally(drx_ref, dxr.at[0], {"cols": right})
        for k in range(1, nx):
            pivot_diag = pivot_diag + drx_ref[k - 1]
        scale = f32(1.0) / jnp.sqrt(pivot_diag)
        rs_ref[...] = jnp.transpose(jnp.broadcast_to(scale, (LANES, batch)))

    ket(1)
    multiply(0)
    x_step(0, 0)
    multiply(1)
    x_step(1, 0)
    ket(2)
    x_step(0, 1)
    multiply(2)
    x_step(2, 0)
    x_step(1, 1)
    ket(3)
    x_step(0, 2)
    multiply(3)
    diag_to_sibling()
    x_step(3, 0)
    x_step(2, 1)
    ket(4)
    x_step(1, 2)
    x_step(0, 3)
    diag_to_band()
    x_step(3, 1)
    x_step(2, 2)
    ket(5)
    x_step(1, 3)
    diag_last()
    finish(0)
    x_step(3, 2)
    x_step(2, 3)
    ket(6)
    finish(1)
    x_step(3, 3)
    ket(7)
    finish(2)
    ket_last()
    finish(3)
    new_ref[...] = jnp.transpose(outt_ref[...]).astype(bf16)
    dout_ref[...] = diag_ref[...] - jnp.sum(squares[0], axis=0, keepdims=True)
    for ref, sem, to in (
        (rx1_ref, p1s, {"rows": up}),
        (rx1_ref, p2s, {"rows": up}),
        (rsib_ref, d2s, {"sub": other}),
        (rxr_ref, xrs, {"cols": right}),
        (rxl_ref, xls, {"cols": left}),
        (krr_ref, krs, {"rows": up}),
        (krl_ref, kls, {"rows": down}),
        (dsib_ref, dss, {"sub": other}),
        (drx_ref, dxs, {"cols": right}),
    ):
        tally(ref, sem.at[0], to, sent=True)


def write_out(new_ref, dout_ref, next_ref, new_hbm, dout_hbm, next_hbm, sem):
    copies = [
        pltpu.make_async_copy(src, dst, sem.at[i])
        for i, (src, dst) in enumerate(
            ((new_ref, new_hbm), (next_ref, next_hbm), (dout_ref, dout_hbm))
        )
    ]
    for copy in copies:
        copy.start()
    for copy in copies:
        copy.wait()


def body(
    nz,
    nx,
    stored_vectors,
    previous_columns,
    pivots,
    diagonal,
    ket_blocks,
    shell_tags,
    target_blocks,
    block_counts,
    shell_norms,
):
    depth, band = stored_vectors.shape
    rows_here, batch = previous_columns.shape
    slots, block_rows, _ = ket_blocks.shape
    blocks = rows_here // block_rows
    chunk = batch // nz
    grows = batch // PIVOT_GROUPS
    wide = -(-(depth + DIAG_PARTS) // LANES) * LANES
    zr, zl = nz // 2, nz - 1 - nz // 2
    half = nx // 2
    x_messages = PIVOT_GROUPS * (nx - 1) // 2
    f32, bf16 = jnp.float32, jnp.bfloat16
    dma = pltpu.SemaphoreType.DMA
    vmem = pl.BlockSpec(memory_space=pltpu.VMEM)
    hbm = pl.BlockSpec(memory_space=pltpu.HBM)
    results = pl.pallas_call(
        functools.partial(kernel, nz, nx),
        out_shape=(
            pltpu.VMEM((rows_here, batch), bf16),
            pltpu.VMEM((1, rows_here), f32),
            pltpu.VMEM((rows_here, batch), bf16),
        ),
        in_specs=[hbm] * 9,
        out_specs=(vmem, vmem, vmem),
        scratch_shapes=[
            pltpu.VMEM((1, batch), jnp.int32),
            pltpu.VMEM((1, rows_here), f32),
            pltpu.VMEM((slots, block_rows), jnp.int32),
            pltpu.SMEM(target_blocks.shape[::-1], jnp.int32),
            pltpu.SMEM(block_counts.shape, jnp.int32),
            pltpu.SMEM(shell_norms.shape, f32),
            pltpu.VMEM((depth, band), bf16),
            pltpu.VMEM((rows_here, batch), bf16),
            pltpu.VMEM((slots, block_rows, batch), bf16),
            pltpu.VMEM((slots, block_rows, batch), bf16),
            pltpu.VMEM((batch, band), bf16),
            pltpu.VMEM((batch, wide), bf16),
            pltpu.VMEM((nz - 1, chunk, wide), bf16),
            pltpu.VMEM((batch, wide), bf16),
            pltpu.VMEM((PIVOT_GROUPS, nx, grows, rows_here), f32),
            pltpu.VMEM((PIVOT_GROUPS, nx, grows, rows_here), f32),
            pltpu.VMEM((PIVOT_GROUPS, nx, grows, rows_here), f32),
            pltpu.VMEM((x_messages, grows, rows_here), f32),
            pltpu.VMEM((x_messages, grows, rows_here), f32),
            pltpu.VMEM((2, blocks, block_rows, batch), bf16),
            pltpu.VMEM((zr, blocks, block_rows, batch), bf16),
            pltpu.VMEM((zl, blocks, block_rows, batch), bf16),
            pltpu.VMEM((1, batch), f32),
            pltpu.VMEM((1, batch), f32),
            pltpu.VMEM((1, batch), f32),
            pltpu.VMEM((nx - 1, 1, batch), f32),
            pltpu.VMEM((batch, rows_here), f32),
            pltpu.VMEM((batch, LANES), f32),
            pltpu.VMEM((batch, rows_here), f32),
            dma((4,)),
            dma((8,)),
            dma((1,)),
            dma((1,)),
            dma((1,)),
            dma((PIVOT_GROUPS,)),
            dma((1,)),
            dma((PIVOT_GROUPS, half)),
            dma((1,)),
            dma((x_messages,)),
            dma((1,)),
            dma((x_messages,)),
            dma((1,)),
            dma((zr, blocks)),
            dma((1,)),
            dma((zl, blocks)),
            dma((1,)),
            dma((1,)),
            dma((1,)),
            dma((1,)),
        ],
        compiler_params=pltpu.CompilerParams(
            collective_id=0, has_side_effects=True, vmem_limit_bytes=24 * 1024 * 1024
        ),
        name="downdate",
    )(
        *(
            pltpu.with_memory_space_constraint(x, pltpu.HBM)
            for x in (
                stored_vectors,
                previous_columns,
                pivots.reshape(1, batch),
                diagonal.reshape(1, rows_here),
                ket_blocks,
                shell_tags,
                target_blocks.T,
                block_counts,
                shell_norms,
            )
        )
    )
    new_vectors, diag_out, next_columns = pl.pallas_call(
        write_out,
        out_shape=(
            pltpu.HBM((rows_here, batch), bf16),
            pltpu.HBM((1, rows_here), f32),
            pltpu.HBM((rows_here, batch), bf16),
        ),
        in_specs=[vmem] * 3,
        out_specs=(hbm, hbm, hbm),
        scratch_shapes=[dma((3,))],
        name="write_out",
    )(*(pltpu.with_memory_space_constraint(x, pltpu.VMEM) for x in results))
    return new_vectors, diag_out.reshape(rows_here), next_columns


def solution(mesh):
    return jax.shard_map(
        functools.partial(body, mesh.shape["rows"], mesh.shape["cols"]),
        mesh=mesh,
        in_specs=(
            P(("cols", "sub"), ("groups", "rows")),
            P(("groups", "rows", "cols", "sub"), None),
            P("groups"),
            P(("groups", "rows", "cols", "sub")),
            P(("groups", "rows", "cols", "sub"), None, None),
            P(("groups", "rows", "cols", "sub"), None),
            P("groups", None),
            P("groups"),
            P(),
        ),
        out_specs=(
            P(("groups", "rows", "cols", "sub"), None),
            P(("groups", "rows", "cols", "sub")),
            P(("groups", "rows", "cols", "sub"), None),
        ),
        check_vma=False,
    )
```

```python
import functools

import jax
import jax.numpy as jnp
from jax import lax
from jax.experimental import pallas as pl
from jax.experimental.pallas import tpu as pltpu
from jax.sharding import PartitionSpec as P

MESH = pl.DeviceIdType.MESH
LANES = 128
PIVOT_GROUPS = 4
DIAG_PARTS = 3
BEFORE = 2


def kernel(
    nz,
    nx,
    v_hbm,
    prev_hbm,
    piv_hbm,
    diag_hbm,
    ket_hbm,
    tags_hbm,
    tgt_hbm,
    cnt_hbm,
    norms_hbm,
    new_ref,
    dout_ref,
    next_ref,
    piv_ref,
    diag_ref,
    tags_ref,
    tgt_ref,
    cnt_ref,
    norms_ref,
    v_ref,
    prev_ref,
    ket_ref,
    fresh_ref,
    hot_ref,
    pick_ref,
    rx1_ref,
    pful_ref,
    snd_ref,
    loc_ref,
    rsib_ref,
    rxr_ref,
    rxl_ref,
    k0_ref,
    n1_ref,
    krr_ref,
    krl_ref,
    dsnd_ref,
    dsib_ref,
    dsum_ref,
    drx_ref,
    prevt_ref,
    rs_ref,
    outt_ref,
    vsem,
    lsem,
    p1s,
    p1r,
    p2s,
    p2r,
    d2s,
    d2r,
    xrs,
    xrr,
    xls,
    xlr,
    krs,
    krq,
    kls,
    klq,
    dss,
    dsr,
    dxs,
    dxr,
):
    f32, bf16 = jnp.float32, jnp.bfloat16
    depth, band = v_ref.shape
    rows_here, batch = prev_ref.shape
    slots, block_rows = ket_ref.shape[0], ket_ref.shape[1]
    blocks = rows_here // block_rows
    chunk = batch // nz
    per = nz // PIVOT_GROUPS
    grows = per * chunk
    half = nx // 2
    r, c, s = lax.axis_index("rows"), lax.axis_index("cols"), lax.axis_index("sub")
    other = 1 - s
    device = (r * nx + c) * 2 + s
    right, left = lax.rem(c + 1, nx), lax.rem(c + nx - 1, nx)
    up, down = lax.rem(r + 1, nz), lax.rem(r + nz - 1, nz)

    def zpeer(k):
        return lax.rem(r + k, nz)

    def xpeer(k):
        return lax.rem(c + k, nx)

    smalls = [
        pltpu.make_async_copy(src, dst, lsem.at[2 + i])
        for i, (src, dst) in enumerate(
            (
                (piv_hbm, piv_ref),
                (diag_hbm, diag_ref),
                (tags_hbm, tags_ref),
                (tgt_hbm, tgt_ref),
                (cnt_hbm, cnt_ref),
                (norms_hbm, norms_ref),
            )
        )
    ]
    for copy in smalls:
        copy.start()
    pieces = 4
    width = band // pieces
    vload = [
        pltpu.make_async_copy(
            v_hbm.at[:, pl.ds(i * width, width)], v_ref.at[:, pl.ds(i * width, width)], vsem.at[i]
        )
        for i in range(pieces)
    ]
    for copy in vload:
        copy.start()
    ketload = pltpu.make_async_copy(ket_hbm, ket_ref, lsem.at[0])
    ketload.start()
    prevload = pltpu.make_async_copy(prev_hbm, prev_ref, lsem.at[1])
    prevload.start()

    barrier = pltpu.get_barrier_semaphore()
    by_reach = sorted(range(1, nz), key=lambda k: -min(k, nz - k))
    for k in by_reach:
        pl.semaphore_signal(barrier, inc=1, device_id={"rows": zpeer(k)}, device_id_type=MESH)
    for k in range(1, nx):
        pl.semaphore_signal(barrier, inc=1, device_id={"cols": xpeer(k)}, device_id_type=MESH)
    pl.semaphore_signal(barrier, inc=1, device_id={"sub": other}, device_id_type=MESH)

    for copy in smalls[:2]:
        copy.wait()
    pivot_cols = jnp.transpose(jnp.broadcast_to(piv_ref[...], (LANES, batch)))
    lane = lax.broadcasted_iota(jnp.int32, (batch, LANES), 1)
    in_band = pivot_cols - r * band - lane
    for t in range(band // LANES):
        hot = jnp.where(in_band == t * LANES, f32(1.0), f32(0.0)).astype(bf16)
        hot_ref[:, t * LANES : (t + 1) * LANES] = hot
    in_device = pivot_cols - device * rows_here - lane
    found = jnp.zeros((batch, LANES), f32)
    for t in range(rows_here // LANES):
        row = diag_ref[:, t * LANES : (t + 1) * LANES]
        found = found + jnp.where(in_device == t * LANES, row, f32(0.0))
    own_diag = jnp.sum(found, axis=1, keepdims=True)
    part_hi = own_diag.astype(bf16).astype(f32)
    part_mid = (own_diag - part_hi).astype(bf16).astype(f32)
    part_lo = own_diag - part_hi - part_mid
    spare = pick_ref.shape[1] - depth
    place = lax.broadcasted_iota(jnp.int32, (batch, spare), 1)
    extra = jnp.where(place == 0, part_hi, f32(0.0))
    extra = jnp.where(place == 1, part_mid, extra)
    extra = jnp.where(place == 2, part_lo, extra)
    pick_ref[:, depth:] = extra.astype(bf16)
    picked = jnp.zeros((batch, depth), f32)
    for i in range(pieces):
        vload[i].wait()
        span = slice(i * width, (i + 1) * width)
        picked = picked + lax.dot_general(
            hot_ref[:, span], v_ref[:, span], (((1,), (1,)), ((), ())), preferred_element_type=f32
        )
    pick_ref[:, :depth] = picked.astype(bf16)

    pl.semaphore_wait(barrier, nz - 1 + nx - 1 + 1)

    def push(src, dst, send_sem, recv_sem, to):
        copy = pltpu.make_async_remote_copy(
            src_ref=src,
            dst_ref=dst,
            send_sem=send_sem,
            recv_sem=recv_sem,
            device_id=to,
            device_id_type=MESH,
        )
        copy.start()

    def tally(ref, sem, to, sent=False):
        copy = pltpu.make_async_remote_copy(
            src_ref=ref,
            dst_ref=ref,
            send_sem=sem,
            recv_sem=sem,
            device_id=to,
            device_id_type=MESH,
        )
        if sent:
            copy.wait_send()
        else:
            copy.wait_recv()

    for k in by_reach:
        to = zpeer(k)
        start = pl.multiple_of(to * chunk, chunk)
        push(
            pick_ref.at[pl.ds(start, chunk), :], rx1_ref.at[k - 1], p1s.at[0], p1r.at[0], {"rows": to}
        )

    ketload.wait()
    for copy in smalls[2:]:
        copy.wait()
    tags = tags_ref[...]
    factor = jnp.zeros(tags.shape, f32)
    for kind in range(norms_ref.shape[0]):
        factor = jnp.where(tags == kind, norms_ref[kind], factor)
    for t in range(slots):
        column = jnp.transpose(jnp.broadcast_to(factor[t : t + 1, :], (LANES, block_rows)))
        for h in range(batch // LANES):
            span = slice(h * LANES, (h + 1) * LANES)
            fresh_ref[t, :, span] = (ket_ref[t, :, span].astype(f32) * column).astype(bf16)
    prevload.wait()
    prevt_ref[...] = jnp.transpose(prev_ref[...].astype(f32))

    targets = [jnp.where(t < cnt_ref[device], tgt_ref[t, device], -1) for t in range(slots)]

    def with_own(value, reach, w):
        block = ((lax.rem(r + reach + nz, nz) * nx + c) * 2 + s) * blocks + w
        slot, hit = 0, targets[0] == block
        for t in range(1, slots):
            slot = jnp.where(targets[t] == block, t, slot)
            hit = hit | (targets[t] == block)
        return jnp.where(hit, fresh_ref[slot], value)

    zr, zl = nz // 2, nz - 1 - nz // 2

    def chain(i, way):
        last, buf, stage, ss, rs, k = (
            (zr, krr_ref, 0, krs, krq, 1) if way > 0 else (zl, krl_ref, 1, kls, klq, nz - 1)
        )
        if i >= last:
            return
        to = {"rows": zpeer(k)}
        reach = way * (last - i)
        if i == 0:
            src = k0_ref.at[stage, 0]
            value = jnp.zeros(fresh_ref.shape[1:], bf16)
            for w in range(blocks):
                value = with_own(value, reach, w)
            src[...] = value
            push(src, buf.at[0], ss.at[0], rs.at[0], to)
            return
        if i == 1:
            tally(buf.at[0], rs.at[0], to)
            first = buf[0]
            before = (zpeer(nz - k) * nx + c) * 2 + s
            theirs = [
                jnp.where(t < cnt_ref[before], tgt_ref[t, before], -1) for t in range(slots)
            ]
        for w in range(blocks):
            goes = 1 + (i - 1) * blocks + w
            if i == 1:
                block = ((lax.rem(r + reach + nz, nz) * nx + c) * 2 + s) * blocks + w
                value = jnp.zeros(fresh_ref.shape[1:], bf16)
                for t in range(slots):
                    value = jnp.where(theirs[t] == block, first, value)
                src = n1_ref.at[stage, w]
            else:
                src = buf.at[goes - blocks]
                tally(src, rs.at[goes - blocks], to)
                value = src[...]
            src[...] = with_own(value, reach, w)
            push(src, buf.at[goes], ss.at[0], rs.at[goes], to)

    def ket(i):
        chain(i, 1)
        chain(i, -1)

    def ket_last():
        for w in range(blocks):
            end_r, end_l = 1 + (zr - 2) * blocks + w, 1 + (zl - 2) * blocks + w
            tally(krr_ref.at[end_r], krq.at[end_r], {"rows": up})
            tally(krl_ref.at[end_l], klq.at[end_l], {"rows": down})
            both = krr_ref[end_r].astype(f32) + krl_ref[end_l].astype(f32)
            next_ref[w * block_rows : (w + 1) * block_rows, :] = with_own(both.astype(bf16), 0, w)

    ket(0)
    ket(1)

    quarter = nz // 4

    def pass_on(src, k, to):
        p = (BEFORE - k) % nz
        sem = PIVOT_GROUPS + (1 if k == quarter else 0) if k in (quarter, nz - quarter) else p // per
        push(src, pful_ref.at[pl.ds(p * chunk, chunk), :], p2s.at[0], p2r.at[sem], {"rows": to})

    def broadcast():
        for k in reversed(by_reach):
            if min(k, nz - k) <= quarter:
                pass_on(pful_ref.at[mine, :], k, zpeer(k))

    def relay():
        for i, (k, hops_on) in enumerate(
            ((nz - quarter, range(-1, -quarter, -1)), (quarter, range(1, quarter + 1)))
        ):
            held = pful_ref.at[pl.ds(((BEFORE - k) % nz) * chunk, chunk), :]
            tally(held, p2r.at[PIVOT_GROUPS + i], {"rows": up})
            for hop in hops_on:
                pass_on(held, (k + hop) % nz, zpeer(hop % nz))

    mine = slice(BEFORE * chunk, (BEFORE + 1) * chunk)

    own = pl.multiple_of(r * chunk, chunk)
    total = pick_ref[pl.ds(own, chunk), :].astype(f32)
    tally(rx1_ref, p1r.at[0], {"rows": up})
    for k in range(1, nz):
        total = total + rx1_ref[k - 1].astype(f32)
    pful_ref[mine, :] = total.astype(bf16)
    broadcast()
    order = [(half - p // 2) if p % 2 == 0 else (half + (p + 1) // 2) % nx for p in range(nx)]
    where_is = {rel: p for p, rel in enumerate(order)}
    members = [0, 1, PIVOT_GROUPS - 1] + list(range(2, PIVOT_GROUPS - 1))
    pairs = nx // 2

    def columns_of(p, core):
        rel = order[p]
        return pl.multiple_of((xpeer(rel) * 2 + core) * rows_here, rows_here)

    def multiply(g):
        first = members[g] * per
        known = (BEFORE, (BEFORE - quarter) % nz, (BEFORE + quarter) % nz)
        coming = per - sum(first <= p < first + per for p in known)
        tally(pful_ref.at[pl.ds(0, coming * chunk), :], p2r.at[members[g]], {"rows": up})
        lhs = pful_ref[first * chunk : first * chunk + grows, :depth]
        for m in range(pairs):
            for p in (2 * m, 2 * m + 1):
                snd_ref[g, p] = jnp.dot(
                    lhs, v_ref[:, pl.ds(columns_of(p, other), rows_here)], preferred_element_type=f32
                )
            span = pl.ds(2 * m, 2)
            push(
                snd_ref.at[g, span], rsib_ref.at[g, span], d2s.at[0], d2r.at[g, m], {"sub": other}
            )
        for p in range(nx):
            loc_ref[g, p] = jnp.dot(
                lhs, v_ref[:, pl.ds(columns_of(p, s), rows_here)], preferred_element_type=f32
            )

    met = set()

    def chip_part(g, p):
        m = p // 2
        if (g, m) not in met:
            met.add((g, m))
            tally(rsib_ref.at[g, pl.ds(2 * m, 2)], d2r.at[g, m], {"sub": other})
        return loc_ref[g, p] + rsib_ref[g, p]

    def hops(g):
        longer = list(range(half, 0, -1)), list(range(nx - half + 1, nx))
        shorter = list(range(half - 1, 0, -1)), list(range(nx - half, nx))
        return longer if g % 2 == 0 else shorter

    def spot(g, way, i):
        return sum(len(hops(q)[way]) for q in range(g)) + i

    def x_step(g, i):
        for way, (buf, ss, rs, to) in enumerate(
            ((rxr_ref, xrs, xrr, right), (rxl_ref, xls, xlr, left))
        ):
            path = hops(g)[way]
            if i >= len(path):
                continue
            p = where_is[path[i]]
            value = chip_part(g, p)
            if i > 0:
                came = spot(g, way, i - 1)
                tally(buf.at[came], rs.at[came], {"cols": to})
                value = value + buf[came]
            loc_ref[g, p] = value
            goes = spot(g, way, i)
            push(loc_ref.at[g, p], buf.at[goes], ss.at[0], rs.at[goes], {"cols": to})

    squares = [jnp.zeros((chunk, rows_here), f32)]

    def finish(g):
        value = chip_part(g, where_is[0])
        for way, (buf, ss, rs, to) in enumerate(
            ((rxr_ref, xrs, xrr, right), (rxl_ref, xls, xlr, left))
        ):
            last = spot(g, way, len(hops(g)[way]) - 1)
            tally(buf.at[last], rs.at[last], {"cols": to})
            value = value + buf[last]
        for q in range(per):
            p = members[g] * per + q
            at = pl.multiple_of(lax.rem(p + r + nz - BEFORE, nz) * chunk, chunk)
            scale = rs_ref[p * chunk : (p + 1) * chunk, :]
            scale = jnp.concatenate([scale] * (rows_here // LANES), axis=1)
            scaled = (prevt_ref[pl.ds(at, chunk), :] - value[q * chunk : (q + 1) * chunk]) * scale
            squares[0] = squares[0] + scaled * scaled
            outt_ref[pl.ds(at, chunk), :] = scaled

    def diag_to_sibling():
        tile = depth // LANES
        at = depth - tile * LANES
        turned = jnp.transpose(pful_ref[:, tile * LANES : (tile + 1) * LANES].astype(f32))
        dsnd_ref[...] = (
            turned[at : at + 1, :] + turned[at + 1 : at + 2, :] + turned[at + 2 : at + 3, :]
        )
        push(dsnd_ref, dsib_ref, dss.at[0], dsr.at[0], {"sub": other})

    def diag_to_band():
        tally(dsib_ref, dsr.at[0], {"sub": other})
        dsum_ref[...] = dsnd_ref[...] + dsib_ref[...]
        for k in range(1, nx):
            push(dsum_ref, drx_ref.at[k - 1], dxs.at[0], dxr.at[0], {"cols": xpeer(k)})

    def diag_last():
        pivot_diag = dsum_ref[...]
        tally(drx_ref, dxr.at[0], {"cols": right})
        for k in range(1, nx):
            pivot_diag = pivot_diag + drx_ref[k - 1]
        scale = f32(1.0) / jnp.sqrt(pivot_diag)
        rs_ref[...] = jnp.transpose(jnp.broadcast_to(scale, (LANES, batch)))

    multiply(0)
    relay()
    x_step(0, 0)
    ket(2)
    multiply(1)
    x_step(1, 0)
    ket(3)
    x_step(0, 1)
    multiply(2)
    x_step(2, 0)
    x_step(1, 1)
    ket(4)
    x_step(0, 2)
    multiply(3)
    diag_to_sibling()
    x_step(3, 0)
    x_step(2, 1)
    ket(5)
    x_step(1, 2)
    x_step(0, 3)
    diag_to_band()
    x_step(3, 1)
    x_step(2, 2)
    ket(6)
    x_step(1, 3)
    diag_last()
    finish(0)
    x_step(3, 2)
    x_step(2, 3)
    ket(7)
    finish(1)
    x_step(3, 3)
    ket(8)
    finish(2)
    ket_last()
    finish(3)
    new_ref[...] = jnp.transpose(outt_ref[...]).astype(bf16)
    dout_ref[...] = diag_ref[...] - jnp.sum(squares[0], axis=0, keepdims=True)
    for ref, sem, to in (
        (rx1_ref, p1s, {"rows": up}),
        (rx1_ref, p2s, {"rows": up}),
        (rsib_ref, d2s, {"sub": other}),
        (rxr_ref, xrs, {"cols": right}),
        (rxl_ref, xls, {"cols": left}),
        (krr_ref, krs, {"rows": up}),
        (krl_ref, kls, {"rows": down}),
        (dsib_ref, dss, {"sub": other}),
        (drx_ref, dxs, {"cols": right}),
    ):
        tally(ref, sem.at[0], to, sent=True)


def write_out(new_ref, dout_ref, next_ref, new_hbm, dout_hbm, next_hbm, sem):
    copies = [
        pltpu.make_async_copy(src, dst, sem.at[i])
        for i, (src, dst) in enumerate(
            ((new_ref, new_hbm), (next_ref, next_hbm), (dout_ref, dout_hbm))
        )
    ]
    for copy in copies:
        copy.start()
    for copy in copies:
        copy.wait()


def body(
    nz,
    nx,
    stored_vectors,
    previous_columns,
    pivots,
    diagonal,
    ket_blocks,
    shell_tags,
    target_blocks,
    block_counts,
    shell_norms,
):
    depth, band = stored_vectors.shape
    rows_here, batch = previous_columns.shape
    slots, block_rows, _ = ket_blocks.shape
    blocks = rows_here // block_rows
    chunk = batch // nz
    grows = batch // PIVOT_GROUPS
    wide = -(-(depth + DIAG_PARTS) // LANES) * LANES
    zr, zl = nz // 2, nz - 1 - nz // 2
    half = nx // 2
    x_messages = PIVOT_GROUPS * (nx - 1) // 2
    f32, bf16 = jnp.float32, jnp.bfloat16
    dma = pltpu.SemaphoreType.DMA
    vmem = pl.BlockSpec(memory_space=pltpu.VMEM)
    hbm = pl.BlockSpec(memory_space=pltpu.HBM)
    results = pl.pallas_call(
        functools.partial(kernel, nz, nx),
        out_shape=(
            pltpu.VMEM((rows_here, batch), bf16),
            pltpu.VMEM((1, rows_here), f32),
            pltpu.VMEM((rows_here, batch), bf16),
        ),
        in_specs=[hbm] * 9,
        out_specs=(vmem, vmem, vmem),
        scratch_shapes=[
            pltpu.VMEM((1, batch), jnp.int32),
            pltpu.VMEM((1, rows_here), f32),
            pltpu.VMEM((slots, block_rows), jnp.int32),
            pltpu.SMEM(target_blocks.shape[::-1], jnp.int32),
            pltpu.SMEM(block_counts.shape, jnp.int32),
            pltpu.SMEM(shell_norms.shape, f32),
            pltpu.VMEM((depth, band), bf16),
            pltpu.VMEM((rows_here, batch), bf16),
            pltpu.VMEM((slots, block_rows, batch), bf16),
            pltpu.VMEM((slots, block_rows, batch), bf16),
            pltpu.VMEM((batch, band), bf16),
            pltpu.VMEM((batch, wide), bf16),
            pltpu.VMEM((nz - 1, chunk, wide), bf16),
            pltpu.VMEM((batch, wide), bf16),
            pltpu.VMEM((PIVOT_GROUPS, nx, grows, rows_here), f32),
            pltpu.VMEM((PIVOT_GROUPS, nx, grows, rows_here), f32),
            pltpu.VMEM((PIVOT_GROUPS, nx, grows, rows_here), f32),
            pltpu.VMEM((x_messages, grows, rows_here), f32),
            pltpu.VMEM((x_messages, grows, rows_here), f32),
            pltpu.VMEM((2, 1, block_rows, batch), bf16),
            pltpu.VMEM((2, blocks, block_rows, batch), bf16),
            pltpu.VMEM((1 + (zr - 1) * blocks, block_rows, batch), bf16),
            pltpu.VMEM((1 + (zl - 1) * blocks, block_rows, batch), bf16),
            pltpu.VMEM((1, batch), f32),
            pltpu.VMEM((1, batch), f32),
            pltpu.VMEM((1, batch), f32),
            pltpu.VMEM((nx - 1, 1, batch), f32),
            pltpu.VMEM((batch, rows_here), f32),
            pltpu.VMEM((batch, LANES), f32),
            pltpu.VMEM((batch, rows_here), f32),
            dma((4,)),
            dma((8,)),
            dma((1,)),
            dma((1,)),
            dma((1,)),
            dma((PIVOT_GROUPS + 2,)),
            dma((1,)),
            dma((PIVOT_GROUPS, half)),
            dma((1,)),
            dma((x_messages,)),
            dma((1,)),
            dma((x_messages,)),
            dma((1,)),
            dma((1 + (zr - 1) * blocks,)),
            dma((1,)),
            dma((1 + (zl - 1) * blocks,)),
            dma((1,)),
            dma((1,)),
            dma((1,)),
            dma((1,)),
        ],
        compiler_params=pltpu.CompilerParams(
            collective_id=0, has_side_effects=True, vmem_limit_bytes=24 * 1024 * 1024
        ),
        name="downdate",
    )(
        *(
            pltpu.with_memory_space_constraint(x, pltpu.HBM)
            for x in (
                stored_vectors,
                previous_columns,
                pivots.reshape(1, batch),
                diagonal.reshape(1, rows_here),
                ket_blocks,
                shell_tags,
                target_blocks.T,
                block_counts,
                shell_norms,
            )
        )
    )
    new_vectors, diag_out, next_columns = pl.pallas_call(
        write_out,
        out_shape=(
            pltpu.HBM((rows_here, batch), bf16),
            pltpu.HBM((1, rows_here), f32),
            pltpu.HBM((rows_here, batch), bf16),
        ),
        in_specs=[vmem] * 3,
        out_specs=(hbm, hbm, hbm),
        scratch_shapes=[dma((3,))],
        name="write_out",
    )(*(pltpu.with_memory_space_constraint(x, pltpu.VMEM) for x in results))
    return new_vectors, diag_out.reshape(rows_here), next_columns


def solution(mesh):
    return jax.shard_map(
        functools.partial(body, mesh.shape["rows"], mesh.shape["cols"]),
        mesh=mesh,
        in_specs=(
            P(("cols", "sub"), ("groups", "rows")),
            P(("groups", "rows", "cols", "sub"), None),
            P("groups"),
            P(("groups", "rows", "cols", "sub")),
            P(("groups", "rows", "cols", "sub"), None, None),
            P(("groups", "rows", "cols", "sub"), None),
            P("groups", None),
            P("groups"),
            P(),
        ),
        out_specs=(
            P(("groups", "rows", "cols", "sub"), None),
            P(("groups", "rows", "cols", "sub")),
            P(("groups", "rows", "cols", "sub"), None),
        ),
        check_vma=False,
    )
```
